32 devices in a mesh: blk: 16 (over z, x, core), col: 2 (over y).
Axes of the slice: x: 2, y: 2, z: 4, core: 2. Of those that a mesh axis runs over, the one named last changes fastest.
Arguments:
- blocks: bfloat16 [16, 2, 2048, 2048], P('blk'), may hold values from -0.09375 to 0.09375
- offsets: int32 [16, 2], P('blk'), may hold values from -2 to 2, as said below
- krylov: bfloat16 [16, 64, 32768], P('col', None, 'blk'), may hold values from -6 to 6
- previous: float32 [64, 16, 32768], P(None, 'col', 'blk')
- node_table: float32 [32], replicated, may hold values from -1.5 to 1.5
- node_index: int32 [16], P('col'), may hold values from 0 to 31
- pole_values: float32 [16], P('col'), may hold values from 4 to 16
- scaling: float32 [16], P('col'), may hold values from 0.5 to 2
Outputs:
- new_basis: bfloat16 [16, 64, 32768], P('col', None, 'blk')
- first_coeffs: float32 [64, 64], replicated
- second_coeffs: float32 [64, 64], replicated
- factor: float32 [64, 64], replicated
The draws below stay inside these ranges and needn't reach their ends.
Inputs may be any that keep to these rules, and one draw needn't show every extreme that they name: `offsets`: each block row's 2 distances are distinct.
All inputs are finite; a program needn't handle non-finite values.
Results may differ from the reference program's by a relative error of at most 0.0012.
Values may be sent and summed in bfloat16 or wider, within the bound.
No kernel may reach another device: no remote copies, remote signals or barrier semaphores. Data moves between devices by JAX's collectives and lax.ppermute only.
A program may use at most 128 MiB of HBM per device.

```python
import math
import jax
import jax.numpy as jnp
from jax import lax

BLOCK_ROWS = 2048
KRYLOV_COLS = 64
TERMS = 16
COUPLINGS = 2
REACH = 2
NODE_COUNT = 32
PREV_COLS = 64
ROWS = 32768
N_BLK = 16


def draw_offsets(key, part):
    width = 2 * REACH + 1
    scores = jax.random.randint(key, (N_BLK, width), 0, 1 << 20) * width + jnp.arange(width, dtype=jnp.int32)[None, :]
    chosen = lax.top_k(scores, COUPLINGS)[1]
    return (chosen - REACH).astype(jnp.int32)


def draw_previous(key, part):
    own_key = jax.random.fold_in(key, 11)
    common_key = jax.random.fold_in(key, 12)
    own = jax.random.normal(own_key, (PREV_COLS, TERMS, ROWS), jnp.float32)
    common = jax.random.normal(common_key, (1, TERMS, ROWS), jnp.float32)
    return (own + 0.125 * common).astype(jnp.float32)


def place_ends(array, stream_key, least, high):
    spot = [jax.random.randint(jax.random.fold_in(stream_key, axis), (), 0, length) for axis, length in enumerate(array.shape)]
    longest = array.shape.index(max(array.shape))
    next_to = spot[:longest] + [(spot[longest] + 1) % array.shape[longest]] + spot[longest + 1:]
    return array.at[tuple(spot)].set(least).at[tuple(next_to)].set(high)


def block_levels(rng, extent, split, low, high):
    factor_of = 1.0
    for axis_at, blocks in split:
        draws = jax.random.uniform(jax.random.fold_in(jax.random.fold_in(rng, 6), axis_at), (blocks,), jnp.float32, low / len(split), high / len(split))
        factor_of = factor_of * jnp.repeat(jnp.exp(draws), extent[axis_at] // blocks).reshape((-1,) + (1,) * (len(extent) - 1 - axis_at))
    return factor_of


def gaussian(rng, shape, scale, reach, cuts=(), kind=jnp.bfloat16):
    entries = scale * jax.random.normal(rng, shape, jnp.float32)
    if cuts:
        entries = entries * block_levels(rng, shape, cuts, -0.22, 0.18)
    return jnp.clip(entries, -reach, reach).astype(kind)


def setup_inputs(seed: int = 0) -> dict:
    arg_keys = jax.random.split(jax.random.key(seed), 9)
    blocks = gaussian(arg_keys[0], (N_BLK, COUPLINGS, BLOCK_ROWS, BLOCK_ROWS), (COUPLINGS * BLOCK_ROWS) ** -0.5, 0.09375, ((0, 16),))
    offsets = draw_offsets(jax.random.fold_in(arg_keys[8], 71), 0)
    krylov = gaussian(arg_keys[2], (TERMS, KRYLOV_COLS, ROWS), 1.0, 6.0, ((0, 2), (2, 16)))
    previous = draw_previous(jax.random.fold_in(arg_keys[8], 71), 0)
    node_table = jnp.clip(jax.random.uniform(arg_keys[4], (NODE_COUNT,), jnp.float32, -1.5, 1.5), -1.5, 1.5)
    node_index = place_ends(jax.random.randint(arg_keys[5], (TERMS,), 0, NODE_COUNT), jax.random.fold_in(arg_keys[5], 1), 0, NODE_COUNT - 1).astype(jnp.int32)
    pole_values = jnp.clip(jnp.exp(math.log(16.0) - 1.3862944 * jax.random.uniform(arg_keys[6], (TERMS,), jnp.float32) ** block_levels(arg_keys[6], (TERMS,), ((0, 2),), -0.2, 0.2)), 4.0, 16.0)
    scaling = jnp.clip(jnp.exp(math.log(2.0) - 1.3862944 * jax.random.uniform(arg_keys[7], (TERMS,), jnp.float32) ** block_levels(arg_keys[7], (TERMS,), ((0, 2),), -0.2, 0.2)), 0.5, 2.0)
    return {"blocks": blocks, "offsets": offsets, "krylov": krylov, "previous": previous, "node_table": node_table, "node_index": node_index, "pole_values": pole_values, "scaling": scaling}


exact_mode = lax.Precision.HIGHEST

def apply_band(blocks, offsets, krylov):
    flat = krylov.reshape(TERMS * KRYLOV_COLS, N_BLK, BLOCK_ROWS)

    def one_row(item):
        position, band, distances = item
        total = jnp.zeros((TERMS * KRYLOV_COLS, BLOCK_ROWS), jnp.float32)
        for coupling in range(COUPLINGS):
            source = ((position + distances[coupling]) % N_BLK).astype(jnp.int32)
            piece = lax.dynamic_index_in_dim(flat, source, 1, keepdims=False)
            total = total + lax.dot_general(piece.astype(jnp.float32), band[coupling].astype(jnp.float32), (((1,), (1,)), ((), ())), preferred_element_type=jnp.float32)
        return total
    image = lax.map(one_row, (jnp.arange(N_BLK, dtype=jnp.int32), blocks, offsets))
    return jnp.transpose(image, (1, 0, 2)).reshape(TERMS, KRYLOV_COLS, N_BLK * BLOCK_ROWS)

def reference(blocks, offsets, krylov, previous, node_table, node_index, pole_values, scaling):
    image = apply_band(blocks, offsets, krylov)
    matches = node_index[:, None] == jnp.arange(NODE_COUNT, dtype=jnp.int32)[None, :]
    shift_value = lax.optimization_barrier(jnp.sum(jnp.where(matches, node_table[None, :], jnp.float32(0.0)), axis=1))
    carry_weight = scaling / (1.0 - shift_value / pole_values)
    before = jnp.concatenate([jnp.zeros_like(krylov[:1]), krylov[:-1]], axis=0)
    work = image - shift_value[:, None, None] * krylov.astype(jnp.float32) + carry_weight[:, None, None] * before.astype(jnp.float32)
    inverse_size = 1.0 / (ROWS * TERMS)
    root_size = math.sqrt(ROWS * TERMS)
    coeff_one = jnp.einsum('ptn,tmn->pm', previous, work, precision=exact_mode) * inverse_size
    first_pass = work - jnp.einsum('ptn,pm->tmn', previous, coeff_one, precision=exact_mode)
    coeff_two = jnp.einsum('ptn,tmn->pm', previous, first_pass, precision=exact_mode) * inverse_size
    second_pass = first_pass - jnp.einsum('ptn,pm->tmn', previous, coeff_two, precision=exact_mode)
    gram = jnp.einsum('tkn,tmn->km', second_pass, second_pass, precision=exact_mode) * inverse_size
    factor = jnp.linalg.cholesky(gram)
    identity = jnp.eye(KRYLOV_COLS, dtype=jnp.float32)
    inverse_factor = jax.scipy.linalg.solve_triangular(factor, identity, lower=True)
    new_basis = jnp.einsum('tkn,mk->tmn', second_pass, inverse_factor, precision=exact_mode).astype(jnp.bfloat16)
    return (new_basis, coeff_one * root_size, coeff_two * root_size, factor)
```

```python
import functools
import math

import jax
import jax.numpy as jnp
from jax import lax
from jax.experimental import pallas as pl
from jax.experimental.pallas import tpu as pltpu
from jax.sharding import PartitionSpec as P

REACH = 2
CHUNKS = 2
WIDTH = 512

exact_mode = lax.Precision.HIGHEST
ROW_DOT = (((1,), (1,)), ((), ()))


def from_behind(block, axis, distance):
    count = lax.axis_size(axis)
    return lax.ppermute(block, axis, [((i - distance) % count, i) for i in range(count)])


def with_partner(block, axis, bit):
    return lax.ppermute(block, axis, [(i ^ bit, i) for i in range(lax.axis_size(axis))])


def passed_along(value, axis):
    count = lax.axis_size(axis)
    return lax.ppermute(value, axis, [(source, source + 1) for source in range(count - 1)])


def summed(value):
    for axis in ("blk", "col"):
        count = lax.axis_size(axis)
        if count & (count - 1):
            value = lax.psum(value, axis)
            continue
        bit = 1
        while bit < count:
            value = value + with_partner(value, axis, bit)
            bit *= 2
    return value


def high_low(value):
    high = value.astype(jnp.bfloat16)
    return high, (value - high.astype(jnp.float32)).astype(jnp.bfloat16)


def folded(gram):
    half = gram.shape[0] // 2
    rows = gram[:half] + gram[half:]
    parts = [
        rows[:, i : i + half] + rows[:, i + half : i + 2 * half]
        for i in range(0, rows.shape[1], 2 * half)
    ]
    return jnp.concatenate(parts, axis=1)


def prepare_kernel(previous_ref, split_ref, gram_ref):
    parts = []
    for t in range(previous_ref.shape[1]):
        high, low = high_low(previous_ref[:, t, :])
        both = jnp.concatenate([high, low], axis=0)
        split_ref[t] = both
        parts.append(both)
    long = jnp.concatenate(parts, axis=1)
    gram_ref[0] = lax.dot_general(long, long, ROW_DOT, preferred_element_type=jnp.float32)


def prepare(previous):
    count, terms, rows = previous.shape
    width = min(WIDTH, rows)
    return pl.pallas_call(
        prepare_kernel,
        grid=(rows // width,),
        in_specs=[pl.BlockSpec((count, terms, width), lambda n: (0, 0, n))],
        out_specs=[
            pl.BlockSpec((terms, 2 * count, width), lambda n: (0, 0, n)),
            pl.BlockSpec((1, 2 * count, 2 * count), lambda n: (n, 0, 0)),
        ],
        out_shape=[
            jax.ShapeDtypeStruct((terms, 2 * count, rows), jnp.bfloat16),
            jax.ShapeDtypeStruct((rows // width, 2 * count, 2 * count), jnp.float32),
        ],
        name="prepare",
    )(previous)


def expand_kernel(
    index_ref, p0, p1, p2, p3, p4, weight_ref, own_ref, before_ref, scale_ref, split_ref,
    *rest, columns, couplings,
):
    work_ref, gram_ref, piece_ref, sems = rest[-4:]
    step = pl.program_id(0)
    terms = split_ref.shape[0]

    @pl.when(step == 0)
    def _():
        for c in range(couplings):
            for k, piece in enumerate((p0, p1, p2, p3, p4)):

                @pl.when(index_ref[c] == k)
                def _(piece=piece, c=c):
                    copy = pltpu.make_async_copy(piece, piece_ref.at[c], sems.at[c])
                    copy.start()

        for c in range(couplings):
            pltpu.make_async_copy(p0, piece_ref.at[c], sems.at[c]).wait()

    total = None
    for c in range(couplings):
        part = lax.dot_general(
            piece_ref[c], weight_ref[0, c], ROW_DOT, preferred_element_type=jnp.float32
        )
        total = part if total is None else total + part
    work = (
        total
        - scale_ref[:, 0:1] * own_ref[...].astype(jnp.float32)
        + scale_ref[:, 1:2] * before_ref[...].astype(jnp.float32)
    )
    high, low = high_low(work)
    parts = []
    for t in range(terms):
        span = slice(t * columns, (t + 1) * columns)
        both = jnp.concatenate([high[span], low[span]], axis=0)
        work_ref[t] = both
        parts.append(both)
    long = jnp.concatenate(parts, axis=1)
    known = jnp.concatenate([split_ref[t] for t in range(terms)], axis=1)
    gram_ref[0] = lax.dot_general(
        long, jnp.concatenate([known, long], axis=0), ROW_DOT, preferred_element_type=jnp.float32
    )


def expand(chunk, chunks, index, pieces, blocks, own, before, scales, split, work):
    couplings, rows = blocks.shape[1], blocks.shape[2]
    terms, double, _ = split.shape
    columns = double // 2
    part = terms // chunks
    high = part * columns
    width = min(WIDTH, rows)
    anywhere = pl.BlockSpec(memory_space=pl.ANY)
    operands = [index, *pieces, blocks, own, before, scales, split]
    in_specs = [
        pl.BlockSpec(memory_space=pltpu.SMEM),
        *[anywhere] * len(pieces),
        pl.BlockSpec((1, couplings, width, rows), lambda n: (0, 0, n, 0)),
        pl.BlockSpec((high, width), lambda n: (chunk, n)),
        pl.BlockSpec((high, width), lambda n: (chunk, n)),
        pl.BlockSpec((high, 2), lambda n: (chunk, 0)),
        pl.BlockSpec((part, double, width), lambda n: (chunk, 0, n)),
    ]
    aliases = {}
    if work is not None:
        aliases = {len(operands): 0}
        operands.append(work)
        in_specs.append(anywhere)
    return pl.pallas_call(
        functools.partial(expand_kernel, columns=columns, couplings=couplings),
        grid=(rows // width,),
        in_specs=in_specs,
        out_specs=[
            pl.BlockSpec((part, double, width), lambda n: (chunk, 0, n)),
            pl.BlockSpec((1, double, 2 * double), lambda n: (n, 0, 0)),
        ],
        out_shape=[
            jax.ShapeDtypeStruct((terms, double, rows), jnp.bfloat16),
            jax.ShapeDtypeStruct((rows // width, double, 2 * double), jnp.float32),
        ],
        scratch_shapes=[
            pltpu.VMEM((couplings, high, rows), jnp.bfloat16),
            pltpu.SemaphoreType.DMA((couplings,)),
        ],
        input_output_aliases=aliases,
        compiler_params=pltpu.CompilerParams(vmem_limit_bytes=48 * 2**20),
        name=f"expand{chunk}",
    )(*operands)


def combine_kernel(mix_ref, work_ref, split_ref, out_ref):
    columns = mix_ref.shape[0]
    high, low = high_low(mix_ref[...])
    mix = jnp.concatenate([high, low], axis=0)
    for t in range(work_ref.shape[0]):
        both = jnp.dot(
            mix,
            jnp.concatenate([work_ref[t], split_ref[t]], axis=0),
            preferred_element_type=jnp.float32,
        )
        out_ref[t] = (both[:columns] + both[columns:]).astype(jnp.bfloat16)


def combine(mix, work, split):
    terms, double, rows = work.shape
    columns = double // 2
    part = 2 if terms % 2 == 0 else 1
    spec = pl.BlockSpec((part, double, rows), lambda t: (t, 0, 0))
    return pl.pallas_call(
        combine_kernel,
        grid=(terms // part,),
        in_specs=[pl.BlockSpec(mix.shape, lambda t: (0, 0)), spec, spec],
        out_specs=pl.BlockSpec((part, columns, rows), lambda t: (t, 0, 0)),
        out_shape=jax.ShapeDtypeStruct((terms, columns, rows), jnp.bfloat16),
        name="combine",
    )(mix, work, split)


def body(blocks, offsets, krylov, previous, node_table, node_index, pole_values, scaling):
    local_terms, columns, local_rows = krylov.shape
    flat = krylov.reshape(local_terms * columns, local_rows)
    chunks = CHUNKS if local_terms % CHUNKS == 0 else 1
    high = flat.shape[0] // chunks
    even = lax.axis_index("blk") % 2 == 0

    parts = [flat[c * high : (c + 1) * high] for c in range(chunks)]
    last_term = passed_along(krylov[-1:], "col")
    beside = [with_partner(part, "blk", 1) for part in parts]
    behind = [from_behind(part, "blk", REACH) for part in parts]
    ahead = [from_behind(part, "blk", -REACH) for part in parts]
    relayed = [
        with_partner(jnp.where(even, a, b), "blk", 1) for a, b in zip(ahead, behind)
    ]

    matches = node_index[:, None] == jnp.arange(node_table.shape[0], dtype=jnp.int32)[None, :]
    shift_value = jnp.sum(jnp.where(matches, node_table[None, :], jnp.float32(0.0)), axis=1)
    carry_weight = scaling / (1.0 - shift_value / pole_values)
    scales = jnp.repeat(jnp.stack([shift_value, carry_weight], axis=1), columns, axis=0)
    before = jnp.concatenate([last_term, krylov[:-1]], axis=0).reshape(flat.shape)

    near = jnp.where(even, 1, -1)
    distance = offsets[0]
    index = jnp.where(
        distance == -REACH,
        0,
        jnp.where(
            distance == REACH,
            1,
            jnp.where(distance == 0, 2, jnp.where(distance == near, 3, 4)),
        ),
    ).astype(jnp.int32)

    split, gram = prepare(previous)
    gram = folded(gram.sum(axis=0))
    half = columns // 2
    total = [jnp.concatenate([gram[:half], gram[half:]], axis=1)]
    work = None
    for c in range(chunks):
        pieces = (behind[c], ahead[c], parts[c], beside[c], relayed[c])
        work, gram = expand(
            c, chunks, index, pieces, blocks, flat, before, scales, split, work
        )
        total.insert(0, folded(gram.sum(axis=0)))

    total_size = local_rows * lax.axis_size("blk") * local_terms * lax.axis_size("col")
    root_size = math.sqrt(total_size)
    local = jnp.concatenate([sum(total[:-1]), total[-1]], axis=0)
    sums = summed(local) * (1.0 / total_size)
    cross = sums[:columns, :columns].T
    self_gram = sums[:columns, columns:]
    packed = sums[columns:]
    basis_gram = jnp.concatenate([packed[:, :columns], packed[:, columns:]], axis=0)
    coeff_two = cross - jnp.dot(basis_gram, cross, precision=exact_mode)
    combined = cross + coeff_two
    mixed = jnp.dot(combined.T, cross, precision=exact_mode)
    inner = jnp.dot(
        combined.T, jnp.dot(basis_gram, combined, precision=exact_mode), precision=exact_mode
    )
    factor = jnp.linalg.cholesky(self_gram - mixed - mixed.T + inner)
    identity = jnp.eye(columns, dtype=jnp.float32)
    inverse_factor = jax.scipy.linalg.solve_triangular(factor, identity, lower=True)
    back = -jnp.dot(inverse_factor, combined.T, precision=exact_mode)
    mix = jnp.concatenate([inverse_factor, inverse_factor, back, back], axis=1)
    new_basis = combine(mix, work, split)
    return (new_basis, cross * root_size, coeff_two * root_size, factor)


def solution(mesh):
    in_specs = (
        P("blk", None, None, None),
        P("blk", None),
        P("col", None, "blk"),
        P(None, "col", "blk"),
        P(),
        P("col"),
        P("col"),
        P("col"),
    )
    out_specs = (P("col", None, "blk"), P(), P(), P())
    return jax.shard_map(body, mesh=mesh, in_specs=in_specs, out_specs=out_specs, check_vma=False)
```

```python
import functools
import math

import jax
import jax.numpy as jnp
from jax import lax
from jax.experimental import pallas as pl
from jax.experimental.pallas import tpu as pltpu
from jax.sharding import PartitionSpec as P

REACH = 2
CHUNKS = 2
WIDTH = 512

exact_mode = lax.Precision.HIGHEST
ROW_DOT = (((1,), (1,)), ((), ()))


def from_behind(block, axis, distance):
    count = lax.axis_size(axis)
    return lax.ppermute(block, axis, [((i - distance) % count, i) for i in range(count)])


def with_partner(block, axis, bit):
    return lax.ppermute(block, axis, [(i ^ bit, i) for i in range(lax.axis_size(axis))])


def passed_along(value, axis):
    count = lax.axis_size(axis)
    return lax.ppermute(value, axis, [(source, source + 1) for source in range(count - 1)])


def summed(value):
    for axis in ("blk", "col"):
        count = lax.axis_size(axis)
        if count & (count - 1):
            value = lax.psum(value, axis)
            continue
        bit = 1
        while bit < count:
            value = value + with_partner(value, axis, bit)
            bit *= 2
    return value


def high_low(value):
    high = value.astype(jnp.bfloat16)
    return high, (value - high.astype(jnp.float32)).astype(jnp.bfloat16)


def folded(gram):
    half = gram.shape[0] // 2
    rows = gram[:half] + gram[half:]
    parts = [
        rows[:, i : i + half] + rows[:, i + half : i + 2 * half]
        for i in range(0, rows.shape[1], 2 * half)
    ]
    return jnp.concatenate(parts, axis=1)


def prepare_kernel(previous_ref, split_ref, gram_ref):
    parts = []
    for t in range(previous_ref.shape[1]):
        high, low = high_low(previous_ref[:, t, :])
        both = jnp.concatenate([high, low], axis=0)
        split_ref[t] = both
        parts.append(both)
    long = jnp.concatenate(parts, axis=1)
    gram_ref[0] = lax.dot_general(long, long, ROW_DOT, preferred_element_type=jnp.float32)


def prepare(previous):
    count, terms, rows = previous.shape
    width = min(WIDTH, rows)
    return pl.pallas_call(
        prepare_kernel,
        grid=(rows // width,),
        in_specs=[pl.BlockSpec((count, terms, width), lambda n: (0, 0, n))],
        out_specs=[
            pl.BlockSpec((terms, 2 * count, width), lambda n: (0, 0, n)),
            pl.BlockSpec((1, 2 * count, 2 * count), lambda n: (n, 0, 0)),
        ],
        out_shape=[
            jax.ShapeDtypeStruct((terms, 2 * count, rows), jnp.bfloat16),
            jax.ShapeDtypeStruct((rows // width, 2 * count, 2 * count), jnp.float32),
        ],
        name="prepare",
    )(previous)


def expand_kernel(
    index_ref, p0, p1, p2, p3, p4, weight_ref, own_ref, before_ref, scale_ref, split_ref,
    *rest, columns, couplings,
):
    work_ref, gram_ref, piece_ref, sems = rest[-4:]
    step = pl.program_id(0)
    terms = split_ref.shape[0]

    @pl.when(step == 0)
    def _():
        for c in range(couplings):
            for k, piece in enumerate((p0, p1, p2, p3, p4)):

                @pl.when(index_ref[c] == k)
                def _(piece=piece, c=c):
                    copy = pltpu.make_async_copy(piece, piece_ref.at[c], sems.at[c])
                    copy.start()

        for c in range(couplings):
            pltpu.make_async_copy(p0, piece_ref.at[c], sems.at[c]).wait()

    total = None
    for c in range(couplings):
        part = lax.dot_general(
            piece_ref[c], weight_ref[0, c], ROW_DOT, preferred_element_type=jnp.float32
        )
        total = part if total is None else total + part
    work = (
        total
        - scale_ref[:, 0:1] * own_ref[...].astype(jnp.float32)
        + scale_ref[:, 1:2] * before_ref[...].astype(jnp.float32)
    )
    high, low = high_low(work)
    parts = []
    for t in range(terms):
        span = slice(t * columns, (t + 1) * columns)
        both = jnp.concatenate([high[span], low[span]], axis=0)
        work_ref[t] = both
        parts.append(both)
    long = jnp.concatenate(parts, axis=1)
    known = jnp.concatenate([split_ref[t] for t in range(terms)], axis=1)
    gram_ref[0] = lax.dot_general(
        long, jnp.concatenate([known, long], axis=0), ROW_DOT, preferred_element_type=jnp.float32
    )


def expand(chunk, chunks, index, pieces, blocks, own, before, scales, split, work):
    couplings, rows = blocks.shape[1], blocks.shape[2]
    terms, double, _ = split.shape
    columns = double // 2
    part = terms // chunks
    high = part * columns
    width = min(WIDTH, rows)
    anywhere = pl.BlockSpec(memory_space=pl.ANY)
    operands = [index, *pieces, blocks, own, before, scales, split]
    in_specs = [
        pl.BlockSpec(memory_space=pltpu.SMEM),
        *[anywhere] * len(pieces),
        pl.BlockSpec((1, couplings, width, rows), lambda n: (0, 0, n, 0)),
        pl.BlockSpec((high, width), lambda n: (chunk, n)),
        pl.BlockSpec((high, width), lambda n: (chunk, n)),
        pl.BlockSpec((high, 2), lambda n: (chunk, 0)),
        pl.BlockSpec((part, double, width), lambda n: (chunk, 0, n)),
    ]
    aliases = {}
    if work is not None:
        aliases = {len(operands): 0}
        operands.append(work)
        in_specs.append(anywhere)
    return pl.pallas_call(
        functools.partial(expand_kernel, columns=columns, couplings=couplings),
        grid=(rows // width,),
        in_specs=in_specs,
        out_specs=[
            pl.BlockSpec((part, double, width), lambda n: (chunk, 0, n)),
            pl.BlockSpec((1, double, 2 * double), lambda n: (n, 0, 0)),
        ],
        out_shape=[
            jax.ShapeDtypeStruct((terms, double, rows), jnp.bfloat16),
            jax.ShapeDtypeStruct((rows // width, double, 2 * double), jnp.float32),
        ],
        scratch_shapes=[
            pltpu.VMEM((couplings, high, rows), jnp.bfloat16),
            pltpu.SemaphoreType.DMA((couplings,)),
        ],
        input_output_aliases=aliases,
        compiler_params=pltpu.CompilerParams(vmem_limit_bytes=48 * 2**20),
        name=f"expand{chunk}",
    )(*operands)


def combine_kernel(mix_ref, work_ref, split_ref, out_ref):
    columns = mix_ref.shape[0]
    high, low = high_low(mix_ref[...])
    mix = jnp.concatenate([high, low], axis=0)
    for t in range(work_ref.shape[0]):
        both = jnp.dot(
            mix,
            jnp.concatenate([work_ref[t], split_ref[t]], axis=0),
            preferred_element_type=jnp.float32,
        )
        out_ref[t] = (both[:columns] + both[columns:]).astype(jnp.bfloat16)


def combine(mix, work, split):
    terms, double, rows = work.shape
    columns = double // 2
    part = 2 if terms % 2 == 0 else 1
    spec = pl.BlockSpec((part, double, rows), lambda t: (t, 0, 0))
    return pl.pallas_call(
        combine_kernel,
        grid=(terms // part,),
        in_specs=[pl.BlockSpec(mix.shape, lambda t: (0, 0)), spec, spec],
        out_specs=pl.BlockSpec((part, columns, rows), lambda t: (t, 0, 0)),
        out_shape=jax.ShapeDtypeStruct((terms, columns, rows), jnp.bfloat16),
        name="combine",
    )(mix, work, split)


def body(blocks, offsets, krylov, previous, node_table, node_index, pole_values, scaling):
    local_terms, columns, local_rows = krylov.shape
    flat = krylov.reshape(local_terms * columns, local_rows)
    chunks = CHUNKS if local_terms % CHUNKS == 0 else 1
    high = flat.shape[0] // chunks
    even = lax.axis_index("blk") % 2 == 0

    parts = [flat[c * high : (c + 1) * high] for c in range(chunks)]
    last_term = passed_along(krylov[-1:], "col")
    beside = [with_partner(part, "blk", 1) for part in parts]
    behind = [from_behind(part, "blk", REACH) for part in parts]
    ahead = [from_behind(part, "blk", -REACH) for part in parts]

    matches = node_index[:, None] == jnp.arange(node_table.shape[0], dtype=jnp.int32)[None, :]
    shift_value = jnp.sum(jnp.where(matches, node_table[None, :], jnp.float32(0.0)), axis=1)
    carry_weight = scaling / (1.0 - shift_value / pole_values)
    scales = jnp.repeat(jnp.stack([shift_value, carry_weight], axis=1), columns, axis=0)
    before = jnp.concatenate([last_term, krylov[:-1]], axis=0).reshape(flat.shape)

    near = jnp.where(even, 1, -1)
    distance = offsets[0]
    index = jnp.where(
        distance == -REACH,
        0,
        jnp.where(
            distance == REACH,
            1,
            jnp.where(distance == 0, 2, jnp.where(distance == near, 3, 4)),
        ),
    ).astype(jnp.int32)

    split, gram = prepare(previous)
    gram = folded(gram.sum(axis=0))
    half = columns // 2
    total = [jnp.concatenate([gram[:half], gram[half:]], axis=1)]
    work = None
    gram = None
    for c in range(chunks):
        if gram is not None:
            behind[c], ahead[c], gram = lax.optimization_barrier((behind[c], ahead[c], gram))
        relayed = with_partner(jnp.where(even, ahead[c], behind[c]), "blk", 1)
        pieces = (behind[c], ahead[c], parts[c], beside[c], relayed)
        work, gram = expand(
            c, chunks, index, pieces, blocks, flat, before, scales, split, work
        )
        total.insert(0, folded(gram.sum(axis=0)))

    total_size = local_rows * lax.axis_size("blk") * local_terms * lax.axis_size("col")
    root_size = math.sqrt(total_size)
    local = jnp.concatenate([sum(total[:-1]), total[-1]], axis=0)
    sums = summed(local) * (1.0 / total_size)
    cross = sums[:columns, :columns].T
    self_gram = sums[:columns, columns:]
    packed = sums[columns:]
    basis_gram = jnp.concatenate([packed[:, :columns], packed[:, columns:]], axis=0)
    coeff_two = cross - jnp.dot(basis_gram, cross, precision=exact_mode)
    combined = cross + coeff_two
    mixed = jnp.dot(combined.T, cross, precision=exact_mode)
    inner = jnp.dot(
        combined.T, jnp.dot(basis_gram, combined, precision=exact_mode), precision=exact_mode
    )
    factor = jnp.linalg.cholesky(self_gram - mixed - mixed.T + inner)
    identity = jnp.eye(columns, dtype=jnp.float32)
    inverse_factor = jax.scipy.linalg.solve_triangular(factor, identity, lower=True)
    back = -jnp.dot(inverse_factor, combined.T, precision=exact_mode)
    mix = jnp.concatenate([inverse_factor, inverse_factor, back, back], axis=1)
    new_basis = combine(mix, work, split)
    return (new_basis, cross * root_size, coeff_two * root_size, factor)


def solution(mesh):
    in_specs = (
        P("blk", None, None, None),
        P("blk", None),
        P("col", None, "blk"),
        P(None, "col", "blk"),
        P(),
        P("col"),
        P("col"),
        P("col"),
    )
    out_specs = (P("col", None, "blk"), P(), P(), P())
    return jax.shard_map(body, mesh=mesh, in_specs=in_specs, out_specs=out_specs, check_vma=False)
```
